128 devices in a mesh: img: 8 (over x, core), slab: 16 (over z, y).
Axes of the slice: x: 4, y: 4, z: 4, core: 2. Of those that a mesh axis runs over, the one named last changes fastest.
Arguments:
- section_input: bfloat16 [1024, 256, 1024], P(('img', 'slab')), parts along dimension 0, may hold values from -54 to 54
- w_reduce: bfloat16 [3, 1024, 256], replicated, may hold values from -0.1875 to 0.1875
- w_spatial: bfloat16 [3, 9, 256, 256], replicated, may hold values from -0.125 to 0.125
- w_expand: bfloat16 [3, 256, 1024], replicated, may hold values from -0.375 to 0.375
- gain_mid: float32 [3, 2, 256], replicated, may hold values from 0.25 to 1.75
- shift_mid: float32 [3, 2, 256], replicated, may hold values from -3 to 3
- gain_out: float32 [3, 1024], replicated, may hold values from 0.25 to 1.75
- shift_out: float32 [3, 1024], replicated, may hold values from -3 to 3
Outputs:
- section_output: bfloat16 [1024, 256, 1024], P(('img', 'slab')), parts along dimension 0
The draws below stay inside these ranges and needn't reach their ends.
There are 8 independent parts, one for each index of `img`. The reference program is written for one: setup_inputs(seed, part) draws one part's arguments, and reference() takes and returns one part's arrays. A program takes and returns all parts, laid end to end along the dimension named above; an argument that names none is the same for every part. Nothing has to cross between parts.
All inputs are finite; a program needn't handle non-finite values.
Results may differ from the reference program's by a relative error of at most 0.01.
Values may be sent and summed in bfloat16 or wider, within the bound.
A program may use at most 128 MiB of HBM per device.

```python
import jax
import jax.numpy as jnp
from jax import lax

C = 1024
CM = 256
W = 256
LAYERS = 3
H = 128


def draw_section_input(key, part):
    positions = jnp.arange(H, dtype=jnp.float32) / max(H - 1, 1)
    noise = jnp.clip(jax.random.normal(key, (H, W, C), jnp.float32), -6.0, 6.0)
    scale = jnp.exp(positions * jnp.log(3.0))
    return (noise * scale[:, None, None]).astype(jnp.bfloat16)


def scatter_about(rng, shape, scale, most, held_as=jnp.bfloat16):
    return jnp.clip(scale * jax.random.normal(rng, shape, jnp.float32), -most, most).astype(held_as)


def setup_inputs(seed: int = 0, part: int = 0) -> dict:
    arg_keys = jax.random.split(jax.random.key(seed), 9)
    part_splits = jax.random.split(jax.random.fold_in(arg_keys[8], part), 9)
    return {
        "section_input": draw_section_input(jax.random.fold_in(jax.random.fold_in(arg_keys[8], part), 71), part),
        "w_reduce": scatter_about(arg_keys[1], (LAYERS, C, CM), C ** -0.5, 0.1875),
        "w_spatial": scatter_about(arg_keys[2], (LAYERS, 9, CM, CM), (9 * CM) ** -0.5, 0.125),
        "w_expand": scatter_about(arg_keys[3], (LAYERS, CM, C), CM ** -0.5, 0.375),
        "gain_mid": jnp.clip(1.0 + 0.15 * jax.random.normal(arg_keys[4], (LAYERS, 2, CM), jnp.float32), 0.25, 1.75),
        "shift_mid": scatter_about(arg_keys[5], (LAYERS, 2, CM), 0.5, 3.0, jnp.float32),
        "gain_out": jnp.clip(1.0 + 0.15 * jax.random.normal(arg_keys[6], (LAYERS, C), jnp.float32), 0.25, 1.75),
        "shift_out": scatter_about(arg_keys[7], (LAYERS, C), 0.5, 3.0, jnp.float32),
    }


def normalize(values, gain, shift):
    mean = lax.optimization_barrier(jnp.mean(values, axis=0))
    var = lax.optimization_barrier(jnp.mean(jnp.square(values - mean), axis=0))
    return (values - mean) * jax.lax.rsqrt(var + 1e-05) * gain + shift

def spatial_conv(hidden, taps):
    rows, width, mid = hidden.shape
    padded = jnp.pad(hidden, ((1, 1), (1, 1), (0, 0)))
    total = jnp.zeros((rows * width, taps.shape[2]), jnp.float32)
    for down in range(3):
        for across in range(3):
            window = padded[down:down + rows, across:across + width].reshape(-1, mid)
            total = total + jnp.dot(window, taps[3 * down + across], preferred_element_type=jnp.float32)
    return total

def reference(section_input, w_reduce, w_spatial, w_expand, gain_mid, shift_mid, gain_out, shift_out):
    rows, width, chans = section_input.shape
    mid = w_reduce.shape[2]
    current = section_input
    for layer in range(LAYERS):
        flat = current.reshape(-1, chans)
        reduced = jnp.dot(flat, w_reduce[layer], preferred_element_type=jnp.float32)
        hidden = jnp.maximum(normalize(reduced, gain_mid[layer, 0], shift_mid[layer, 0]), 0.0).astype(jnp.bfloat16)
        spatial = spatial_conv(hidden.reshape(rows, width, mid), w_spatial[layer])
        inner = jnp.maximum(normalize(spatial, gain_mid[layer, 1], shift_mid[layer, 1]), 0.0).astype(jnp.bfloat16)
        expanded = jnp.dot(inner, w_expand[layer], preferred_element_type=jnp.float32)
        summed = normalize(expanded, gain_out[layer], shift_out[layer]) + flat.astype(jnp.float32)
        current = jnp.maximum(summed, 0.0).astype(jnp.bfloat16).reshape(rows, width, chans)
    return current
```

```python
import functools

import jax
import jax.numpy as jnp
from jax import lax
from jax.experimental import pallas as pl
from jax.experimental.pallas import tpu as pltpu
from jax.sharding import PartitionSpec as P

MESH = pl.DeviceIdType.MESH
F32 = jnp.float32
BF16 = jnp.bfloat16


def row_sums(y):
    m, c = y.shape
    y3 = y.reshape(m // 8, 8, c)
    return jnp.sum(y3, axis=0), jnp.sum(y3 * y3, axis=0)


def kernel(
    n, rows, width, chans, mid, layers,
    x_hbm, wr_hbm, ws_hbm, we_hbm, gm_hbm, sm_hbm, go_hbm, so_hbm,
    out_hbm,
    x, wr, ws, we, gm, sm, go, so,
    red, hid, spa, ex,
    halo_out, halo_in, st_out, st_in, se_out, se_in,
    x_sem, w_sem, p_sem, o_sem, hs_sem, hr_sem, ss_sem, sr_sem, es_sem, er_sem,
):
    me = lax.axis_index("slab")
    count = float(rows * width * n)

    def load(src, dst, sem):
        return pltpu.make_async_copy(src, dst, sem)

    def w_copies(layer):
        return (
            load(wr_hbm.at[layer], wr.at[layer], w_sem.at[0, layer]),
            load(ws_hbm.at[layer], ws.at[layer], w_sem.at[1, layer]),
            load(we_hbm.at[layer], we.at[layer], w_sem.at[2, layer]),
        )

    def x_copy(r):
        return load(x_hbm.at[r], x.at[pl.ds(pl.multiple_of(r * width, width), width)], x_sem.at[r])

    params = ((gm_hbm, gm), (sm_hbm, sm), (go_hbm, go), (so_hbm, so))

    w_copies(0)[0].start()
    for r in range(rows):
        x_copy(r).start()
    for i, (a, b) in enumerate(params):
        load(a, b, p_sem.at[i]).start()
    for layer in range(layers):
        for j, c in enumerate(w_copies(layer)):
            if (layer, j) != (0, 0):
                c.start()

    barrier = pltpu.get_barrier_semaphore()
    for d in range(1, n):
        pl.semaphore_signal(
            barrier, inc=1, device_id={"slab": lax.rem(me + d, n)}, device_id_type=MESH
        )

    def block(r):
        return pl.ds(pl.multiple_of(r * width, width), width)

    def send_all(src, dst, slot, send_sem, recv_sem):
        for d in range(1, n):
            pltpu.make_async_remote_copy(
                src_ref=src.at[slot],
                dst_ref=dst.at[slot, d - 1],
                send_sem=send_sem.at[slot],
                recv_sem=recv_sem.at[slot],
                device_id={"slab": lax.rem(me + d, n)},
                device_id_type=MESH,
            ).start()

    def wait_all(dst, slot, sem):
        pltpu.make_async_copy(dst.at[slot], dst.at[slot], sem.at[slot]).wait()

    def pack(s, q):
        return jnp.concatenate(
            [jnp.sum(s, axis=0, keepdims=True), jnp.sum(q, axis=0, keepdims=True)], axis=0
        )

    def coefficients(own, others, gain, shift):
        total = own
        for d in range(n - 1):
            total = total + others[d]
        mean = total[0:1] / count
        var = jnp.maximum(total[1:2] / count - mean * mean, 0.0)
        alpha = lax.rsqrt(var + 1e-05) * gain
        return alpha, shift - mean * alpha

    def reduce_rows(layer, r):
        y = jnp.dot(x[block(r)], wr[layer], preferred_element_type=F32)
        red[block(r)] = y
        return row_sums(y)

    def add2(c, d):
        return c[0] + d[0], c[1] + d[1]

    zero_mid = (jnp.zeros((8, mid), F32), jnp.zeros((8, mid), F32))
    zero_out = (jnp.zeros((8, chans), F32), jnp.zeros((8, chans), F32))

    w_copies(0)[0].wait()

    def first(r, carry):
        x_copy(r).wait()
        return add2(carry, reduce_rows(0, r))

    carry0 = lax.fori_loop(0, rows, first, zero_mid)

    pl.semaphore_wait(barrier, n - 1)
    for i, (a, b) in enumerate(params):
        load(a, b, p_sem.at[i]).wait()

    def halo_copy(layer, side):
        peer = me - 1 if side == 0 else me + 1
        return pltpu.make_async_remote_copy(
            src_ref=halo_out.at[layer, side],
            dst_ref=halo_in.at[layer, 1 - side],
            send_sem=hs_sem.at[layer, side],
            recv_sem=hr_sem.at[layer, 1 - side],
            device_id={"slab": peer},
            device_id_type=MESH,
        )

    has_side = (me > 0, me < n - 1)

    col = lax.broadcasted_iota(jnp.int32, (width, mid), 0)

    def put_hidden(slot, h):
        dst = block(slot)
        hid[dst, mid : 2 * mid] = h.astype(BF16)
        before = jnp.where(col == 0, 0.0, pltpu.roll(h, 1, 0))
        hid[dst, 0:mid] = before.astype(BF16)
        after = jnp.where(col == width - 1, 0.0, pltpu.roll(h, width - 1, 0))
        hid[dst, 2 * mid : 3 * mid] = after.astype(BF16)

    def layer_body(layer, carry):
        own = pack(*carry)
        k = 2 * layer
        st_out[k] = own
        send_all(st_out, st_in, k, ss_sem, sr_sem)
        local_mean = own[0:1] * (1.0 / (rows * width))
        for side in range(2):
            edge = 0 if side == 0 else rows - 1

            @pl.when(has_side[side])
            def _():
                halo_out[layer, side] = (red[block(edge)] - local_mean).astype(BF16)
                halo_copy(layer, side).start()

        wait_all(st_in, k, sr_sem)
        others = [st_in[k, d] for d in range(n - 1)]
        alpha, beta = coefficients(own, others, gm[layer, 0:1], sm[layer, 0:1])

        def hidden_rows(r, c):
            put_hidden(r + 1, jnp.maximum(red[block(r)] * alpha + beta, 0.0))
            return c

        lax.fori_loop(0, rows, hidden_rows, 0)

        w_copies(layer)[1].wait()

        def conv_row(r, carry):
            y = jnp.dot(hid[block(r)], ws[layer, 0], preferred_element_type=F32)
            y = y + jnp.dot(hid[block(r + 1)], ws[layer, 1], preferred_element_type=F32)
            y = y + jnp.dot(hid[block(r + 2)], ws[layer, 2], preferred_element_type=F32)
            spa[block(r)] = y
            return add2(carry, row_sums(y))

        carry = lax.fori_loop(1, rows - 1, conv_row, zero_mid)

        for side in range(2):
            slot = 0 if side == 0 else rows + 1

            @pl.when(has_side[side])
            def _():
                arrived = halo_in.at[layer, side]
                load(arrived, arrived, hr_sem.at[layer, side]).wait()
                their = others[0 if side == 0 else n - 2][0:1] * (1.0 / (rows * width))
                y = halo_in[layer, side].astype(F32) + their
                put_hidden(slot, jnp.maximum(y * alpha + beta, 0.0))

            @pl.when(jnp.logical_not(has_side[side]))
            def _():
                hid[block(slot)] = jnp.zeros((width, 3 * mid), BF16)

        carry = lax.fori_loop(
            0, 2, lambda i, c: conv_row(i * (rows - 1), c), carry
        )

        own = pack(*carry)
        k = 2 * layer + 1
        st_out[k] = own
        send_all(st_out, st_in, k, ss_sem, sr_sem)
        w_copies(layer)[2].wait()
        wait_all(st_in, k, sr_sem)
        others = [st_in[k, d] for d in range(n - 1)]
        alpha, beta = coefficients(own, others, gm[layer, 1:2], sm[layer, 1:2])

        def expand_rows(r, carry):
            inner = jnp.maximum(spa[block(r)] * alpha + beta, 0.0).astype(BF16)
            y = jnp.dot(inner, we[layer], preferred_element_type=F32)
            ex[block(r)] = y
            return add2(carry, row_sums(y))

        carry = lax.fori_loop(0, rows, expand_rows, zero_out)

        own = pack(*carry)
        se_out[layer] = own
        send_all(se_out, se_in, layer, es_sem, er_sem)
        wait_all(se_in, layer, er_sem)
        others = [se_in[layer, d] for d in range(n - 1)]
        alpha, beta = coefficients(own, others, go[pl.ds(layer, 1)], so[pl.ds(layer, 1)])

        def update(r):
            y = ex[block(r)] * alpha + beta + x[block(r)].astype(F32)
            x[block(r)] = jnp.maximum(y, 0.0).astype(BF16)

        def middle():
            w_copies(layer + 1)[0].wait()

            def body(r, carry):
                update(r)
                return add2(carry, reduce_rows(layer + 1, r))

            return lax.fori_loop(0, rows, body, zero_mid)

        def last():
            def body(r, c):
                update(r)
                load(x.at[block(r)], out_hbm.at[r], o_sem.at[r]).start()
                return c

            lax.fori_loop(0, rows, body, 0)
            return zero_mid

        return lax.cond(layer < layers - 1, middle, last)

    lax.fori_loop(0, layers, layer_body, carry0)

    for r in range(rows):
        load(x.at[block(r)], out_hbm.at[r], o_sem.at[r]).wait()
    for layer in range(layers):
        for side in range(2):

            @pl.when(has_side[side])
            def _():
                halo_copy(layer, side).wait_send()

        wait_all(st_in, 2 * layer, ss_sem)
        wait_all(st_in, 2 * layer + 1, ss_sem)
        wait_all(se_in, layer, es_sem)


def solution(mesh):
    n = mesh.shape["slab"]

    def local(x, w_reduce, w_spatial, w_expand, gain_mid, shift_mid, gain_out, shift_out):
        rows, width, chans = x.shape
        layers, _, mid = w_reduce.shape
        taps = w_spatial.reshape(layers, 3, 3 * mid, mid)
        anywhere = pl.BlockSpec(memory_space=pltpu.HBM)
        size = rows * width
        dma = pltpu.SemaphoreType.DMA
        return pl.pallas_call(
            functools.partial(kernel, n, rows, width, chans, mid, layers),
            out_shape=jax.ShapeDtypeStruct(x.shape, BF16),
            in_specs=[anywhere] * 8,
            out_specs=anywhere,
            scratch_shapes=[
                pltpu.VMEM((size, chans), BF16),
                pltpu.VMEM((layers, chans, mid), BF16),
                pltpu.VMEM((layers, 3, 3 * mid, mid), BF16),
                pltpu.VMEM((layers, mid, chans), BF16),
                pltpu.VMEM((layers, 2, mid), F32),
                pltpu.VMEM((layers, 2, mid), F32),
                pltpu.VMEM((layers, chans), F32),
                pltpu.VMEM((layers, chans), F32),
                pltpu.VMEM((size, mid), F32),
                pltpu.VMEM(((rows + 2) * width, 3 * mid), BF16),
                pltpu.VMEM((size, mid), F32),
                pltpu.VMEM((size, chans), F32),
                pltpu.VMEM((layers, 2, width, mid), BF16),
                pltpu.VMEM((layers, 2, width, mid), BF16),
                pltpu.VMEM((2 * layers, 2, mid), F32),
                pltpu.VMEM((2 * layers, n - 1, 2, mid), F32),
                pltpu.VMEM((layers, 2, chans), F32),
                pltpu.VMEM((layers, n - 1, 2, chans), F32),
                dma((rows,)),
                dma((3, layers)),
                dma((4,)),
                dma((rows,)),
                dma((layers, 2)),
                dma((layers, 2)),
                dma((2 * layers,)),
                dma((2 * layers,)),
                dma((layers,)),
                dma((layers,)),
            ],
            compiler_params=pltpu.CompilerParams(
                collective_id=0, has_side_effects=True, vmem_limit_bytes=60 * 1024 * 1024
            ),
            name="blocks",
        )(x, w_reduce, taps, w_expand, gain_mid, shift_mid, gain_out, shift_out)

    placed = (P(("img", "slab"), None, None), P(), P(), P(), P(), P(), P(), P())
    return jax.shard_map(
        local, mesh=mesh, in_specs=placed, out_specs=P(("img", "slab"), None, None), check_vma=False
    )
```

```python
import functools

import jax
import jax.numpy as jnp
from jax import lax
from jax.experimental import pallas as pl
from jax.experimental.pallas import tpu as pltpu
from jax.sharding import PartitionSpec as P

MESH = pl.DeviceIdType.MESH
F32 = jnp.float32
BF16 = jnp.bfloat16


def row_sums(y):
    m, c = y.shape
    y3 = y.reshape(m // 8, 8, c)
    return jnp.sum(y3, axis=0), jnp.sum(y3 * y3, axis=0)


def kernel(
    n, side_y, rows, width, chans, mid, layers,
    x_hbm, wr_hbm, ws_hbm, we_hbm, gm_hbm, sm_hbm, go_hbm, so_hbm,
    ex, x, last_ab,
    wr, ws, we, gm, sm, go, so,
    red, hid, spa,
    halo_out, halo_in, st_out, st_in, se_out, se_in,
    x_sem, w_sem, p_sem, hs_sem, hr_sem, ss_sem, sr_sem, es_sem, er_sem,
):
    me = lax.axis_index("slab")
    count = float(rows * width * n)

    def load(src, dst, sem):
        return pltpu.make_async_copy(src, dst, sem)

    def w_copies(layer):
        return (
            load(wr_hbm.at[layer], wr.at[layer], w_sem.at[0, layer]),
            load(ws_hbm.at[layer], ws.at[layer], w_sem.at[1, layer]),
            load(we_hbm.at[layer], we.at[layer], w_sem.at[2, layer]),
        )

    def x_copy(r):
        return load(x_hbm.at[r], x.at[pl.ds(pl.multiple_of(r * width, width), width)], x_sem.at[r])

    params = ((gm_hbm, gm), (sm_hbm, sm), (go_hbm, go), (so_hbm, so))

    w_copies(0)[0].start()
    for r in range(rows):
        x_copy(r).start()
    for i, (a, b) in enumerate(params):
        load(a, b, p_sem.at[i]).start()
    for layer in range(layers):
        for j, c in enumerate(w_copies(layer)):
            if (layer, j) != (0, 0):
                c.start()

    barrier = pltpu.get_barrier_semaphore()
    for d in range(1, n):
        pl.semaphore_signal(
            barrier, inc=1, device_id={"slab": lax.rem(me + d, n)}, device_id_type=MESH
        )

    def block(r):
        if isinstance(r, int):
            return pl.ds(r * width, width)
        return pl.ds(pl.multiple_of(r * width, width), width)

    def slot_of(side):
        y = lax.rem(me, side_y)
        if side == 0:
            wraps = y == 0
            return jnp.where(wraps, 1 * side_y + 1, 1) - 1
        wraps = y == side_y - 1
        return jnp.where(wraps, n - 1, side_y - 1) - 1

    def distance(d):
        return sum(min(c, side - c) for c, side in ((d // side_y, n // side_y), (d % side_y, side_y)))

    far_first = sorted(range(1, n), key=lambda d: (-distance(d), d))

    def peer(d):
        z, y = me // side_y, me % side_y
        return lax.rem(z + d // side_y, n // side_y) * side_y + lax.rem(y + d % side_y, side_y)

    def send_all(src, dst, slot, send_sem, recv_sem):
        for d in far_first:
            pltpu.make_async_remote_copy(
                src_ref=src.at[slot],
                dst_ref=dst.at[slot, d - 1],
                send_sem=send_sem.at[slot],
                recv_sem=recv_sem.at[slot],
                device_id={"slab": peer(d)},
                device_id_type=MESH,
            ).start()

    def wait_all(dst, slot, sem):
        pltpu.make_async_copy(dst.at[slot], dst.at[slot], sem.at[slot]).wait()

    def pack(s, q):
        return jnp.concatenate(
            [jnp.sum(s, axis=0, keepdims=True), jnp.sum(q, axis=0, keepdims=True)], axis=0
        )

    def coefficients(own, others, gain, shift):
        total = own
        for d in range(n - 1):
            total = total + others[d]
        mean = total[0:1] / count
        var = jnp.maximum(total[1:2] / count - mean * mean, 0.0)
        alpha = lax.rsqrt(var + 1e-05) * gain
        return alpha, shift - mean * alpha

    def reduce_rows(layer, r):
        y = jnp.dot(x[block(r)], wr[layer], preferred_element_type=F32)
        red[block(r)] = y
        return row_sums(y)

    def add2(c, d):
        return c[0] + d[0], c[1] + d[1]

    zero_mid = (jnp.zeros((8, mid), F32), jnp.zeros((8, mid), F32))
    zero_out = (jnp.zeros((8, chans), F32), jnp.zeros((8, chans), F32))

    w_copies(0)[0].wait()

    def first(r, carry):
        x_copy(r).wait()
        return add2(carry, reduce_rows(0, r))

    carry0 = lax.fori_loop(0, rows, first, zero_mid)

    pl.semaphore_wait(barrier, n - 1)
    for i, (a, b) in enumerate(params):
        load(a, b, p_sem.at[i]).wait()

    def halo_copy(layer, side):
        peer = me - 1 if side == 0 else me + 1
        return pltpu.make_async_remote_copy(
            src_ref=halo_out.at[layer, side],
            dst_ref=halo_in.at[layer, 1 - side],
            send_sem=hs_sem.at[layer, side],
            recv_sem=hr_sem.at[layer, 1 - side],
            device_id={"slab": peer},
            device_id_type=MESH,
        )

    has_side = (me > 0, me < n - 1)
    for side in range(2):

        @pl.when(jnp.logical_not(has_side[side]))
        def _():
            for layer in range(layers):
                halo_in[layer, side] = jnp.zeros((width, mid), BF16)

    col = lax.broadcasted_iota(jnp.int32, (width, mid), 0)

    def put_hidden(slot, h):
        dst = block(slot)
        hid[dst, mid : 2 * mid] = h.astype(BF16)
        before = jnp.where(col == 0, 0.0, pltpu.roll(h, 1, 0))
        hid[dst, 0:mid] = before.astype(BF16)
        after = jnp.where(col == width - 1, 0.0, pltpu.roll(h, width - 1, 0))
        hid[dst, 2 * mid : 3 * mid] = after.astype(BF16)

    def layer_body(layer, carry):
        own = pack(*carry)
        k = 2 * layer
        st_out[k] = own
        send_all(st_out, st_in, k, ss_sem, sr_sem)
        local_mean = own[0:1] * (1.0 / (rows * width))
        for side in range(2):
            edge = 0 if side == 0 else rows - 1

            halo_out[layer, side] = (red[block(edge)] - local_mean).astype(BF16)

            @pl.when(has_side[side])
            def _():
                halo_copy(layer, side).start()

        wait_all(st_in, k, sr_sem)
        others = [st_in[k, d] for d in range(n - 1)]
        alpha, beta = coefficients(own, others, gm[layer, 0:1], sm[layer, 0:1])

        w_copies(layer)[1].wait()

        def hidden_row(r):
            put_hidden(r + 1, jnp.maximum(red[block(r)] * alpha + beta, 0.0))

        def conv_row(r, carry):
            y = jnp.dot(hid[block(r + 1)], ws[layer, 1], preferred_element_type=F32)
            if r > 0:
                y = y + jnp.dot(hid[block(r)], ws[layer, 0], preferred_element_type=F32)
                y = y + jnp.dot(hid[block(r + 2)], ws[layer, 2], preferred_element_type=F32)
            else:
                y = y + jnp.dot(hid[block(r + 2)], ws[layer, 2], preferred_element_type=F32)
                y = y + jnp.dot(hid[block(r)], ws[layer, 0], preferred_element_type=F32)
            spa[block(r)] = y
            return add2(carry, row_sums(y))

        hidden_row(0)
        hidden_row(1)
        carry = zero_mid
        for r in range(1, rows - 1):
            hidden_row(r + 1)
            carry = conv_row(r, carry)

        for side in range(2):

            @pl.when(has_side[side])
            def _():
                arrived = halo_in.at[layer, side]
                load(arrived, arrived, hr_sem.at[layer, side]).wait()

        for side in range(2):
            their = st_in[k, slot_of(side)][0:1] * (1.0 / (rows * width))
            y = halo_in[layer, side].astype(F32) + their
            h = jnp.maximum(y * alpha + beta, 0.0)
            put_hidden(0 if side == 0 else rows + 1, jnp.where(has_side[side], h, 0.0))
        carry = conv_row(0, carry)
        carry = conv_row(rows - 1, carry)

        own = pack(*carry)
        k = 2 * layer + 1
        st_out[k] = own
        send_all(st_out, st_in, k, ss_sem, sr_sem)
        w_copies(layer)[2].wait()
        wait_all(st_in, k, sr_sem)
        others = [st_in[k, d] for d in range(n - 1)]
        alpha, beta = coefficients(own, others, gm[layer, 1:2], sm[layer, 1:2])

        def expand_rows(r, carry):
            inner = jnp.maximum(spa[block(r)] * alpha + beta, 0.0).astype(BF16)
            y = jnp.dot(inner, we[layer], preferred_element_type=F32)
            ex[block(r)] = y
            return add2(carry, row_sums(y))

        carry = zero_out
        for r in range(rows):
            carry = expand_rows(r, carry)

        own = pack(*carry)
        se_out[layer] = own
        send_all(se_out, se_in, layer, es_sem, er_sem)
        wait_all(se_in, layer, er_sem)
        others = [se_in[layer, d] for d in range(n - 1)]
        alpha, beta = coefficients(own, others, go[pl.ds(layer, 1)], so[pl.ds(layer, 1)])

        def update(r):
            y = ex[block(r)] * alpha + beta + x[block(r)].astype(F32)
            x[block(r)] = jnp.maximum(y, 0.0).astype(BF16)

        def middle():
            w_copies(layer + 1)[0].wait()
            carry = zero_mid
            for r in range(rows):
                update(r)
                carry = add2(carry, reduce_rows(layer + 1, r))
            return carry

        def last():
            last_ab[0:1] = alpha
            last_ab[1:2] = beta
            return zero_mid

        return lax.cond(layer < layers - 1, middle, last)

    lax.fori_loop(0, layers, layer_body, carry0)

    for layer in range(layers):
        for side in range(2):

            @pl.when(has_side[side])
            def _():
                halo_copy(layer, side).wait_send()

        wait_all(st_in, 2 * layer, ss_sem)
        wait_all(st_in, 2 * layer + 1, ss_sem)
        wait_all(se_in, layer, es_sem)


def finish(rows, width, ex, x, ab, out_hbm, out, sem):
    alpha, beta = ab[0:1], ab[1:2]
    for r in range(rows):
        at = pl.ds(r * width, width)
        y = ex[at] * alpha + beta + x[at].astype(F32)
        out[at] = jnp.maximum(y, 0.0).astype(BF16)
        pltpu.make_async_copy(out.at[at], out_hbm.at[r], sem.at[r]).start()
    for r in range(rows):
        at = pl.ds(r * width, width)
        pltpu.make_async_copy(out.at[at], out_hbm.at[r], sem.at[r]).wait()


def solution(mesh):
    n = mesh.shape["slab"]
    side_y = 4 if n % 4 == 0 else 1

    def local(x, w_reduce, w_spatial, w_expand, gain_mid, shift_mid, gain_out, shift_out):
        rows, width, chans = x.shape
        layers, _, mid = w_reduce.shape
        taps = w_spatial.reshape(layers, 3, 3 * mid, mid)
        anywhere = pl.BlockSpec(memory_space=pltpu.HBM)
        in_vmem = pl.BlockSpec(memory_space=pltpu.VMEM)
        size = rows * width
        dma = pltpu.SemaphoreType.DMA
        ex, last_x, ab = pl.pallas_call(
            functools.partial(kernel, n, side_y, rows, width, chans, mid, layers),
            out_shape=(
                pltpu.VMEM((size, chans), F32),
                pltpu.VMEM((size, chans), BF16),
                pltpu.VMEM((2, chans), F32),
            ),
            in_specs=[anywhere] * 8,
            out_specs=(in_vmem, in_vmem, in_vmem),
            scratch_shapes=[
                pltpu.VMEM((layers, chans, mid), BF16),
                pltpu.VMEM((layers, 3, 3 * mid, mid), BF16),
                pltpu.VMEM((layers, mid, chans), BF16),
                pltpu.VMEM((layers, 2, mid), F32),
                pltpu.VMEM((layers, 2, mid), F32),
                pltpu.VMEM((layers, chans), F32),
                pltpu.VMEM((layers, chans), F32),
                pltpu.VMEM((size, mid), F32),
                pltpu.VMEM(((rows + 2) * width, 3 * mid), BF16),
                pltpu.VMEM((size, mid), F32),
                pltpu.VMEM((layers, 2, width, mid), BF16),
                pltpu.VMEM((layers, 2, width, mid), BF16),
                pltpu.VMEM((2 * layers, 2, mid), F32),
                pltpu.VMEM((2 * layers, n - 1, 2, mid), F32),
                pltpu.VMEM((layers, 2, chans), F32),
                pltpu.VMEM((layers, n - 1, 2, chans), F32),
                dma((rows,)),
                dma((3, layers)),
                dma((4,)),
                dma((layers, 2)),
                dma((layers, 2)),
                dma((2 * layers,)),
                dma((2 * layers,)),
                dma((layers,)),
                dma((layers,)),
            ],
            compiler_params=pltpu.CompilerParams(
                collective_id=0, has_side_effects=True, vmem_limit_bytes=54_400_000
            ),
            name="blocks",
        )(x, w_reduce, taps, w_expand, gain_mid, shift_mid, gain_out, shift_out)
        return pl.pallas_call(
            functools.partial(finish, rows, width),
            out_shape=jax.ShapeDtypeStruct(x.shape, BF16),
            in_specs=[in_vmem] * 3,
            out_specs=anywhere,
            scratch_shapes=[pltpu.VMEM((size, chans), BF16), dma((rows,))],
            compiler_params=pltpu.CompilerParams(vmem_limit_bytes=24 * 1024 * 1024),
            name="finish",
        )(ex, last_x, ab)

    placed = (P(("img", "slab"), None, None), P(), P(), P(), P(), P(), P(), P())
    return jax.shard_map(
        local, mesh=mesh, in_specs=placed, out_specs=P(("img", "slab"), None, None), check_vma=False
    )
```

```python
import functools

import jax
import jax.numpy as jnp
from jax import lax
from jax.experimental import pallas as pl
from jax.experimental.pallas import tpu as pltpu
from jax.sharding import PartitionSpec as P

MESH = pl.DeviceIdType.MESH
F32 = jnp.float32
BF16 = jnp.bfloat16


def row_sums(y):
    m, c = y.shape
    y3 = y.reshape(m // 8, 8, c)
    return jnp.sum(y3, axis=0), jnp.sum(y3 * y3, axis=0)


def kernel(
    n, side_y, rows, width, chans, mid, layers,
    x_hbm, wr_hbm, ws_hbm, we_hbm, gm_hbm, sm_hbm, go_hbm, so_hbm,
    ex, x, last_ab,
    wr, ws, we, gm, sm, go, so,
    red, hid, spa, wt, prod,
    halo_out, halo_in, st_out, st_in, se_out, se_in,
    x_sem, w_sem, p_sem, hs_sem, hr_sem, ss_sem, sr_sem, es_sem, er_sem,
):
    me = lax.axis_index("slab")
    count = float(rows * width * n)

    def load(src, dst, sem):
        return pltpu.make_async_copy(src, dst, sem)

    def w_copies(layer):
        return (
            load(wr_hbm.at[layer], wr.at[layer], w_sem.at[0, layer]),
            load(ws_hbm.at[layer], ws.at[layer], w_sem.at[1, layer]),
            load(we_hbm.at[layer], we.at[layer], w_sem.at[2, layer]),
        )

    def x_copy(r):
        return load(x_hbm.at[r], x.at[pl.ds(pl.multiple_of(r * width, width), width)], x_sem.at[r])

    params = ((gm_hbm, gm), (sm_hbm, sm), (go_hbm, go), (so_hbm, so))

    w_copies(0)[0].start()
    for r in range(2):
        x_copy(r).start()
    for i, (a, b) in enumerate(params):
        load(a, b, p_sem.at[i]).start()
    barrier = pltpu.get_barrier_semaphore()
    for d in range(1, n):
        pl.semaphore_signal(
            barrier, inc=1, device_id={"slab": lax.rem(me + d, n)}, device_id_type=MESH
        )
    pl.delay(500)
    for r in range(2, rows):
        x_copy(r).start()

    def block(r):
        if isinstance(r, int):
            return pl.ds(r * width, width)
        return pl.ds(pl.multiple_of(r * width, width), width)

    def slot_of(side):
        y = lax.rem(me, side_y)
        if side == 0:
            wraps = y == 0
            return jnp.where(wraps, 1 * side_y + 1, 1) - 1
        wraps = y == side_y - 1
        return jnp.where(wraps, n - 1, side_y - 1) - 1

    def distance(d):
        return sum(min(c, side - c) for c, side in ((d // side_y, n // side_y), (d % side_y, side_y)))

    far_first = sorted(range(1, n), key=lambda d: (-distance(d), d))

    def peer(d):
        z, y = me // side_y, me % side_y
        return lax.rem(z + d // side_y, n // side_y) * side_y + lax.rem(y + d % side_y, side_y)

    def send_all(src, dst, slot, send_sem, recv_sem):
        for d in far_first:
            pltpu.make_async_remote_copy(
                src_ref=src.at[slot],
                dst_ref=dst.at[slot, d - 1],
                send_sem=send_sem.at[slot],
                recv_sem=recv_sem.at[slot],
                device_id={"slab": peer(d)},
                device_id_type=MESH,
            ).start()

    def wait_all(dst, slot, sem):
        pltpu.make_async_copy(dst.at[slot], dst.at[slot], sem.at[slot]).wait()

    def pack(s, q):
        return jnp.concatenate(
            [jnp.sum(s, axis=0, keepdims=True), jnp.sum(q, axis=0, keepdims=True)], axis=0
        )

    def coefficients(own, others, gain, shift):
        total = own
        for d in range(n - 1):
            total = total + others[d]
        mean = total[0:1] / count
        var = jnp.maximum(total[1:2] / count - mean * mean, 0.0)
        alpha = lax.rsqrt(var + 1e-05) * gain
        return alpha, shift - mean * alpha

    def reduce_rows(layer, r):
        y = jnp.dot(x[block(r)], wr[layer], preferred_element_type=F32)
        red[block(r)] = y
        return row_sums(y)

    def add2(c, d):
        return c[0] + d[0], c[1] + d[1]

    zero_mid = (jnp.zeros((8, mid), F32), jnp.zeros((8, mid), F32))
    zero_out = (jnp.zeros((8, chans), F32), jnp.zeros((8, chans), F32))

    w_copies(0)[0].wait()

    def first(i, carry):
        x_copy(2 * i).wait()
        x_copy(2 * i + 1).wait()
        carry = add2(carry, reduce_rows(0, 2 * i))
        return add2(carry, reduce_rows(0, 2 * i + 1))

    carry0 = lax.fori_loop(0, rows // 2, first, zero_mid)

    for layer in range(layers):
        for j, c in enumerate(w_copies(layer)):
            if (layer, j) != (0, 0):
                c.start()

    pl.semaphore_wait(barrier, n - 1)
    for i, (a, b) in enumerate(params):
        load(a, b, p_sem.at[i]).wait()

    def halo_copy(layer, side):
        peer = me - 1 if side == 0 else me + 1
        return pltpu.make_async_remote_copy(
            src_ref=halo_out.at[layer, side],
            dst_ref=halo_in.at[layer, 1 - side],
            send_sem=hs_sem.at[layer, side],
            recv_sem=hr_sem.at[layer, 1 - side],
            device_id={"slab": peer},
            device_id_type=MESH,
        )

    has_side = (me > 0, me < n - 1)
    for side in range(2):

        @pl.when(jnp.logical_not(has_side[side]))
        def _():
            for layer in range(layers):
                halo_in[layer, side] = jnp.zeros((width, mid), BF16)

    row8 = lax.broadcasted_iota(jnp.int32, (8, mid), 0)

    def put_hidden(slot, h):
        dst = block(slot)
        hid[dst, mid : 2 * mid] = h.astype(BF16)
        before = pltpu.roll(h, 1, 0)
        edge = jnp.where(row8 == 0, 0.0, before[:8])
        hid[dst, 0:mid] = jnp.concatenate([edge, before[8:]], axis=0).astype(BF16)
        after = pltpu.roll(h, width - 1, 0)
        edge = jnp.where(row8 == 7, 0.0, after[-8:])
        hid[dst, 2 * mid : 3 * mid] = jnp.concatenate([after[:-8], edge], axis=0).astype(BF16)

    def layer_body(layer, carry):
        own = pack(*carry)
        k = 2 * layer
        st_out[k] = own
        send_all(st_out, st_in, k, ss_sem, sr_sem)
        local_mean = own[0:1] * (1.0 / (rows * width))
        for side in range(2):
            edge = 0 if side == 0 else rows - 1

            halo_out[layer, side] = (red[block(edge)] - local_mean).astype(BF16)

            @pl.when(has_side[side])
            def _():
                halo_copy(layer, side).start()

        w_copies(layer)[1].wait()

        @pl.loop(0, 3 * mid // 64)
        def _(i):
            at = pl.ds(pl.multiple_of(i * 64, 64), 64)
            outer = ws[layer, 0, at].astype(F32) + ws[layer, 2, at].astype(F32)
            inner = ws[layer, 1, at].astype(F32)
            wt[0, at] = (0.5 * (outer + inner)).astype(BF16)
            wt[1, at] = (0.5 * (outer - inner)).astype(BF16)

        wait_all(st_in, k, sr_sem)
        others = [st_in[k, d] for d in range(n - 1)]
        alpha, beta = coefficients(own, others, gm[layer, 0:1], sm[layer, 0:1])

        def hidden_row(r):
            put_hidden(r + 1, jnp.maximum(red[block(r)] * alpha + beta, 0.0))

        def conv_pair(r, carry):
            d0, d1, d2, d3 = (hid[block(r + i)] for i in range(4))
            prod[0] = jnp.dot(d1 + d2, wt[0], preferred_element_type=F32)
            prod[1] = jnp.dot(d2 - d1, wt[1], preferred_element_type=F32)
            y = jnp.dot(d0 - d2, ws[layer, 0], preferred_element_type=F32)
            y = y + (prod[0] + prod[1])
            spa[block(r)] = y
            carry = add2(carry, row_sums(y))
            y = jnp.dot(d3 - d1, ws[layer, 2], preferred_element_type=F32)
            y = y + (prod[0] - prod[1])
            spa[block(r + 1)] = y
            return add2(carry, row_sums(y))

        for r in range(1, 5):
            hidden_row(r)
        carry = conv_pair(2, zero_mid)
        hidden_row(5)
        hidden_row(6)
        carry = conv_pair(4, carry)
        hidden_row(0)
        hidden_row(7)

        for side in range(2):

            @pl.when(has_side[side])
            def _():
                arrived = halo_in.at[layer, side]
                load(arrived, arrived, hr_sem.at[layer, side]).wait()

        for side in range(2):
            their = st_in[k, slot_of(side)][0:1] * (1.0 / (rows * width))
            y = halo_in[layer, side].astype(F32) + their
            h = jnp.maximum(y * alpha + beta, 0.0)
            put_hidden(0 if side == 0 else rows + 1, jnp.where(has_side[side], h, 0.0))
        carry = conv_pair(0, carry)
        carry = conv_pair(rows - 2, carry)

        own = pack(*carry)
        k = 2 * layer + 1
        st_out[k] = own
        send_all(st_out, st_in, k, ss_sem, sr_sem)
        w_copies(layer)[2].wait()
        wait_all(st_in, k, sr_sem)
        others = [st_in[k, d] for d in range(n - 1)]
        alpha, beta = coefficients(own, others, gm[layer, 1:2], sm[layer, 1:2])

        def expand_rows(r, carry):
            inner = jnp.maximum(spa[block(r)] * alpha + beta, 0.0).astype(BF16)
            y = jnp.dot(inner, we[layer], preferred_element_type=F32)
            ex[block(r)] = y
            return add2(carry, row_sums(y))

        carry = zero_out
        for r in range(rows):
            carry = expand_rows(r, carry)

        own = pack(*carry)
        se_out[layer] = own
        send_all(se_out, se_in, layer, es_sem, er_sem)
        wait_all(se_in, layer, er_sem)
        others = [se_in[layer, d] for d in range(n - 1)]
        alpha, beta = coefficients(own, others, go[pl.ds(layer, 1)], so[pl.ds(layer, 1)])

        def update(r):
            y = (ex[block(r)] * alpha + beta).astype(BF16) + x[block(r)]
            x[block(r)] = jnp.maximum(y, jnp.zeros_like(y))

        def middle():
            w_copies(layer + 1)[0].wait()
            carry = zero_mid
            for r in range(rows):
                update(r)
                carry = add2(carry, reduce_rows(layer + 1, r))
            return carry

        def last():
            last_ab[0:1] = alpha
            last_ab[1:2] = beta
            return zero_mid

        return lax.cond(layer < layers - 1, middle, last)

    lax.fori_loop(0, layers, layer_body, carry0)

    for layer in range(layers):
        for side in range(2):

            @pl.when(has_side[side])
            def _():
                halo_copy(layer, side).wait_send()

        wait_all(st_in, 2 * layer, ss_sem)
        wait_all(st_in, 2 * layer + 1, ss_sem)
        wait_all(se_in, layer, es_sem)


def finish(rows, width, ex, x, ab, out_hbm, out, sem):
    alpha, beta = ab[0:1], ab[1:2]
    for r in range(rows):
        at = pl.ds(r * width, width)
        y = (ex[at] * alpha + beta).astype(BF16) + x[at]
        out[at] = jnp.maximum(y, jnp.zeros_like(y))
        pltpu.make_async_copy(out.at[at], out_hbm.at[r], sem.at[r]).start()
    for r in range(rows):
        at = pl.ds(r * width, width)
        pltpu.make_async_copy(out.at[at], out_hbm.at[r], sem.at[r]).wait()


def solution(mesh):
    n = mesh.shape["slab"]
    side_y = 4 if n % 4 == 0 else 1

    def local(x, w_reduce, w_spatial, w_expand, gain_mid, shift_mid, gain_out, shift_out):
        rows, width, chans = x.shape
        layers, _, mid = w_reduce.shape
        taps = w_spatial.reshape(layers, 3, 3 * mid, mid)
        anywhere = pl.BlockSpec(memory_space=pltpu.HBM)
        in_vmem = pl.BlockSpec(memory_space=pltpu.VMEM)
        size = rows * width
        dma = pltpu.SemaphoreType.DMA
        ex, last_x, ab = pl.pallas_call(
            functools.partial(kernel, n, side_y, rows, width, chans, mid, layers),
            out_shape=(
                pltpu.VMEM((size, chans), F32),
                pltpu.VMEM((size, chans), BF16),
                pltpu.VMEM((2, chans), F32),
            ),
            in_specs=[anywhere] * 8,
            out_specs=(in_vmem, in_vmem, in_vmem),
            scratch_shapes=[
                pltpu.VMEM((layers, chans, mid), BF16),
                pltpu.VMEM((layers, 3, 3 * mid, mid), BF16),
                pltpu.VMEM((layers, mid, chans), BF16),
                pltpu.VMEM((layers, 2, mid), F32),
                pltpu.VMEM((layers, 2, mid), F32),
                pltpu.VMEM((layers, chans), F32),
                pltpu.VMEM((layers, chans), F32),
                pltpu.VMEM((size, mid), F32),
                pltpu.VMEM(((rows + 2) * width, 3 * mid), BF16),
                pltpu.VMEM((size, mid), F32),
                pltpu.VMEM((2, 3 * mid, mid), BF16),
                pltpu.VMEM((2, width, mid), F32),
                pltpu.VMEM((layers, 2, width, mid), BF16),
                pltpu.VMEM((layers, 2, width, mid), BF16),
                pltpu.VMEM((2 * layers, 2, mid), F32),
                pltpu.VMEM((2 * layers, n - 1, 2, mid), F32),
                pltpu.VMEM((layers, 2, chans), F32),
                pltpu.VMEM((layers, n - 1, 2, chans), F32),
                dma((rows,)),
                dma((3, layers)),
                dma((4,)),
                dma((layers, 2)),
                dma((layers, 2)),
                dma((2 * layers,)),
                dma((2 * layers,)),
                dma((layers,)),
                dma((layers,)),
            ],
            compiler_params=pltpu.CompilerParams(
                collective_id=0, has_side_effects=True, vmem_limit_bytes=54_400_000
            ),
            name="blocks",
        )(x, w_reduce, taps, w_expand, gain_mid, shift_mid, gain_out, shift_out)
        return pl.pallas_call(
            functools.partial(finish, rows, width),
            out_shape=jax.ShapeDtypeStruct(x.shape, BF16),
            in_specs=[in_vmem] * 3,
            out_specs=anywhere,
            scratch_shapes=[pltpu.VMEM((size, chans), BF16), dma((rows,))],
            compiler_params=pltpu.CompilerParams(vmem_limit_bytes=24 * 1024 * 1024),
            name="finish",
        )(ex, last_x, ab)

    placed = (P(("img", "slab"), None, None), P(), P(), P(), P(), P(), P(), P())
    return jax.shard_map(
        local, mesh=mesh, in_specs=placed, out_specs=P(("img", "slab"), None, None), check_vma=False
    )
```

```python
import functools

import jax
import jax.numpy as jnp
from jax import lax
from jax.experimental import pallas as pl
from jax.experimental.pallas import tpu as pltpu
from jax.sharding import PartitionSpec as P

MESH = pl.DeviceIdType.MESH
F32 = jnp.float32
BF16 = jnp.bfloat16
GROUPS = 2


def row_sums(y):
    m, c = y.shape
    y3 = y.reshape(m // 8, 8, c)
    return jnp.sum(y3, axis=0), jnp.sum(y3 * y3, axis=0)


def kernel(
    n, side_y, rows, width, chans, mid, layers,
    x_hbm, wr_hbm, ws_hbm, we_hbm, gm_hbm, sm_hbm, go_hbm, so_hbm,
    ex, x, last_ab,
    wr, ws, we, gm, sm, go, so,
    red, hid, spa, inn, wt, prod,
    halo_out, halo_in, st_out, st_in, se_out, se_in,
    x_sem, w_sem, p_sem, hs_sem, hr_sem, ss_sem, sr_sem, es_sem, er_sem,
):
    me = lax.axis_index("slab")
    count = float(rows * width * n)

    def load(src, dst, sem):
        return pltpu.make_async_copy(src, dst, sem)

    def w_copies(layer):
        return (
            load(wr_hbm.at[layer], wr.at[layer], w_sem.at[0, layer]),
            load(ws_hbm.at[layer], ws.at[layer], w_sem.at[1, layer]),
            load(we_hbm.at[layer], we.at[layer], w_sem.at[2, layer]),
        )

    def x_copy(r):
        return load(x_hbm.at[r], x.at[pl.ds(pl.multiple_of(r * width, width), width)], x_sem.at[r])

    params = ((gm_hbm, gm), (sm_hbm, sm), (go_hbm, go), (so_hbm, so))

    w_copies(0)[0].start()
    early = 3 * rows // 8
    for r in range(early):
        x_copy(r).start()
    for i, (a, b) in enumerate(params):
        load(a, b, p_sem.at[i]).start()
    barrier = pltpu.get_barrier_semaphore()
    for d in range(1, n):
        pl.semaphore_signal(
            barrier, inc=1, device_id={"slab": lax.rem(me + d, n)}, device_id_type=MESH
        )
    pl.delay(300)
    for r in range(early, rows):
        x_copy(r).start()

    def block(r):
        if isinstance(r, int):
            return pl.ds(r * width, width)
        return pl.ds(pl.multiple_of(r * width, width), width)

    def slot_of(side):
        y = lax.rem(me, side_y)
        if side == 0:
            wraps = y == 0
            return jnp.where(wraps, 1 * side_y + 1, 1) - 1
        wraps = y == side_y - 1
        return jnp.where(wraps, n - 1, side_y - 1) - 1

    def distance(d):
        return sum(min(c, side - c) for c, side in ((d // side_y, n // side_y), (d % side_y, side_y)))

    far_first = sorted(range(1, n), key=lambda d: (-distance(d), d))

    def peer(d):
        z, y = me // side_y, me % side_y
        return lax.rem(z + d // side_y, n // side_y) * side_y + lax.rem(y + d % side_y, side_y)

    def send_all(src, dst, slot, send_sem, recv_sem):
        for d in far_first:
            pltpu.make_async_remote_copy(
                src_ref=src.at[slot],
                dst_ref=dst.at[slot, d - 1],
                send_sem=send_sem.at[slot],
                recv_sem=recv_sem.at[slot],
                device_id={"slab": peer(d)},
                device_id_type=MESH,
            ).start()

    def wait_all(dst, slot, sem):
        pltpu.make_async_copy(dst.at[slot], dst.at[slot], sem.at[slot]).wait()

    def pack(s, q):
        return jnp.concatenate(
            [jnp.sum(s, axis=0, keepdims=True), jnp.sum(q, axis=0, keepdims=True)], axis=0
        )

    def coefficients(own, others, gain, shift):
        total = own
        for d in range(n - 1):
            total = total + others[d]
        mean = total[0:1] / count
        var = jnp.maximum(total[1:2] / count - mean * mean, 0.0)
        alpha = lax.rsqrt(var + 1e-05) * gain
        return alpha, shift - mean * alpha

    def reduce_rows(layer, r):
        y = jnp.dot(x[block(r)], wr[layer], preferred_element_type=F32)
        red[block(r)] = y
        return row_sums(y)

    def add2(c, d):
        return c[0] + d[0], c[1] + d[1]

    zero_mid = (jnp.zeros((8, mid), F32), jnp.zeros((8, mid), F32))
    cols = chans // GROUPS
    zero_out = (jnp.zeros((8, cols), F32), jnp.zeros((8, cols), F32))

    def group(g):
        return pl.ds(g * cols, cols)

    w_copies(0)[0].wait()

    carry0 = zero_mid
    for part in (range(early), range(early, rows)):
        for r in part:
            x_copy(r).wait()
        for r in part:
            carry0 = add2(carry0, reduce_rows(0, r))

    for layer in range(layers):
        for j, c in enumerate(w_copies(layer)):
            if (layer, j) != (0, 0):
                c.start()

    pl.semaphore_wait(barrier, n - 1)
    for i, (a, b) in enumerate(params):
        load(a, b, p_sem.at[i]).wait()

    def halo_copy(layer, side):
        peer = me - 1 if side == 0 else me + 1
        return pltpu.make_async_remote_copy(
            src_ref=halo_out.at[layer, side],
            dst_ref=halo_in.at[layer, 1 - side],
            send_sem=hs_sem.at[layer, side],
            recv_sem=hr_sem.at[layer, 1 - side],
            device_id={"slab": peer},
            device_id_type=MESH,
        )

    has_side = (me > 0, me < n - 1)
    for side in range(2):

        @pl.when(jnp.logical_not(has_side[side]))
        def _():
            for layer in range(layers):
                halo_in[layer, side] = jnp.zeros((width, mid), BF16)

    row8 = lax.broadcasted_iota(jnp.int32, (8, mid), 0)

    def put_hidden(slot, h):
        dst = block(slot)
        hid[dst, mid : 2 * mid] = h.astype(BF16)
        before = pltpu.roll(h, 1, 0)
        edge = jnp.where(row8 == 0, 0.0, before[:8])
        hid[dst, 0:mid] = jnp.concatenate([edge, before[8:]], axis=0).astype(BF16)
        after = pltpu.roll(h, width - 1, 0)
        edge = jnp.where(row8 == 7, 0.0, after[-8:])
        hid[dst, 2 * mid : 3 * mid] = jnp.concatenate([after[:-8], edge], axis=0).astype(BF16)

    def layer_body(layer, carry):
        own = pack(*carry)
        k = 2 * layer
        st_out[k] = own
        send_all(st_out, st_in, k, ss_sem, sr_sem)
        local_mean = own[0:1] * (1.0 / (rows * width))
        for side in range(2):
            edge = 0 if side == 0 else rows - 1

            halo_out[layer, side] = (red[block(edge)] - local_mean).astype(BF16)

            @pl.when(has_side[side])
            def _():
                halo_copy(layer, side).start()

        w_copies(layer)[1].wait()

        @pl.loop(0, 3 * mid // 64)
        def _(i):
            at = pl.ds(pl.multiple_of(i * 64, 64), 64)
            outer = ws[layer, 0, at].astype(F32) + ws[layer, 2, at].astype(F32)
            inner = ws[layer, 1, at].astype(F32)
            wt[0, at] = (0.5 * (outer + inner)).astype(BF16)
            wt[1, at] = (0.5 * (outer - inner)).astype(BF16)

        wait_all(st_in, k, sr_sem)
        others = [st_in[k, d] for d in range(n - 1)]
        alpha, beta = coefficients(own, others, gm[layer, 0:1], sm[layer, 0:1])

        def hidden_row(r):
            put_hidden(r + 1, jnp.maximum(red[block(r)] * alpha + beta, 0.0))

        def finish_row(r, carry, lhs, taps, rest):
            y = jnp.dot(lhs, taps, preferred_element_type=F32) + rest
            spa[block(r)] = y
            return add2(carry, row_sums(y))

        hidden_row(0)
        hidden_row(1)
        carry = zero_mid
        for r in range(0, rows, 2):
            a, b = r % 4, r % 4 + 1
            d1, d2 = hid[block(r + 1)], hid[block(r + 2)]
            prod[a] = jnp.dot(d1 + d2, wt[0], preferred_element_type=F32)
            prod[b] = jnp.dot(d2 - d1, wt[1], preferred_element_type=F32)
            if r + 2 < rows:
                hidden_row(r + 2)
                hidden_row(r + 3)
            both = prod[a] + prod[b]
            if r > 0:
                carry = finish_row(r, carry, hid[block(r)] - d2, ws[layer, 0], both)
            else:
                spa[block(r)] = both
            both = prod[a] - prod[b]
            if r + 2 < rows:
                carry = finish_row(r + 1, carry, hid[block(r + 3)] - d1, ws[layer, 2], both)
            else:
                spa[block(r + 1)] = both

        for side in range(2):

            @pl.when(has_side[side])
            def _():
                arrived = halo_in.at[layer, side]
                load(arrived, arrived, hr_sem.at[layer, side]).wait()

        for side in range(2):
            their = st_in[k, slot_of(side)][0:1] * (1.0 / (rows * width))
            y = halo_in[layer, side].astype(F32) + their
            h = jnp.maximum(y * alpha + beta, 0.0)
            put_hidden(0 if side == 0 else rows + 1, jnp.where(has_side[side], h, 0.0))
        lhs = hid[block(0)] - hid[block(2)]
        carry = finish_row(0, carry, lhs, ws[layer, 0], spa[block(0)])
        lhs = hid[block(rows + 1)] - hid[block(rows - 1)]
        carry = finish_row(rows - 1, carry, lhs, ws[layer, 2], spa[block(rows - 1)])

        own = pack(*carry)
        k = 2 * layer + 1
        st_out[k] = own
        send_all(st_out, st_in, k, ss_sem, sr_sem)
        w_copies(layer)[2].wait()
        wait_all(st_in, k, sr_sem)
        others = [st_in[k, d] for d in range(n - 1)]
        alpha, beta = coefficients(own, others, gm[layer, 1:2], sm[layer, 1:2])

        def expand_row(r, g, carry):
            if g == 0:
                inn[block(r)] = jnp.maximum(spa[block(r)] * alpha + beta, 0.0).astype(BF16)
            y = jnp.dot(inn[block(r)], we[layer, :, group(g)], preferred_element_type=F32)
            ex[block(r), group(g)] = y
            return add2(carry, row_sums(y))

        sums = []
        for g in range(GROUPS):
            carry = zero_out
            for r in range(rows):
                carry = expand_row(r, g, carry)
            own = pack(*carry)
            sums.append(own)
            slot = GROUPS * layer + g
            se_out[slot] = own
            send_all(se_out, se_in, slot, es_sem, er_sem)

        carry = zero_mid
        for g in range(GROUPS):
            slot = GROUPS * layer + g
            wait_all(se_in, slot, er_sem)
            others = [se_in[slot, d] for d in range(n - 1)]
            at_layer = pl.ds(layer, 1)
            scale, offset = coefficients(
                sums[g], others, go[at_layer, group(g)], so[at_layer, group(g)]
            )

            def update(r):
                y = (ex[block(r), group(g)] * scale + offset).astype(BF16) + x[block(r), group(g)]
                x[block(r), group(g)] = jnp.maximum(y, jnp.zeros_like(y))

            def middle():
                if g == 0:
                    w_copies(layer + 1)[0].wait()
                carry = zero_mid
                for r in range(rows):
                    update(r)
                    taps = wr[layer + 1, group(g)]
                    y = jnp.dot(x[block(r), group(g)], taps, preferred_element_type=F32)
                    if g > 0:
                        y = y + red[block(r)]
                    red[block(r)] = y
                    if g == GROUPS - 1:
                        carry = add2(carry, row_sums(y))
                return carry

            def last():
                if g < GROUPS - 1:
                    for r in range(rows):
                        update(r)
                else:
                    last_ab[0:1] = scale
                    last_ab[1:2] = offset
                return zero_mid

            carry = lax.cond(layer < layers - 1, middle, last)
        return carry

    lax.fori_loop(0, layers, layer_body, carry0)

    for layer in range(layers):
        for side in range(2):

            @pl.when(has_side[side])
            def _():
                halo_copy(layer, side).wait_send()

        wait_all(st_in, 2 * layer, ss_sem)
        wait_all(st_in, 2 * layer + 1, ss_sem)
        for g in range(GROUPS):
            wait_all(se_in, GROUPS * layer + g, es_sem)


def finish(rows, width, ex, x, ab, out_hbm, out, sem, done_sem):
    alpha, beta = ab[0:1], ab[1:2]
    cols = ab.shape[1]
    done = ex.shape[1] - cols
    ready, left = pl.ds(0, done), pl.ds(done, cols)
    copies = []
    for r in range(rows):
        src = x.at[pl.ds(r * width, width), ready]
        copies.append(pltpu.make_async_copy(src, out_hbm.at[r, :, ready], done_sem.at[r]))
        copies[-1].start()
    for r in range(rows):
        at = pl.ds(r * width, width)
        y = (ex[at, left] * alpha + beta).astype(BF16) + x[at, left]
        out[at] = jnp.maximum(y, jnp.zeros_like(y))
        copies.append(pltpu.make_async_copy(out.at[at], out_hbm.at[r, :, left], sem.at[r]))
        copies[-1].start()
    for copy in copies:
        copy.wait()


def solution(mesh):
    n = mesh.shape["slab"]
    side_y = 4 if n % 4 == 0 else 1

    def local(x, w_reduce, w_spatial, w_expand, gain_mid, shift_mid, gain_out, shift_out):
        rows, width, chans = x.shape
        layers, _, mid = w_reduce.shape
        taps = w_spatial.reshape(layers, 3, 3 * mid, mid)
        anywhere = pl.BlockSpec(memory_space=pltpu.HBM)
        in_vmem = pl.BlockSpec(memory_space=pltpu.VMEM)
        size = rows * width
        dma = pltpu.SemaphoreType.DMA
        ex, last_x, ab = pl.pallas_call(
            functools.partial(kernel, n, side_y, rows, width, chans, mid, layers),
            out_shape=(
                pltpu.VMEM((size, chans), F32),
                pltpu.VMEM((size, chans), BF16),
                pltpu.VMEM((2, chans // GROUPS), F32),
            ),
            in_specs=[anywhere] * 8,
            out_specs=(in_vmem, in_vmem, in_vmem),
            scratch_shapes=[
                pltpu.VMEM((layers, chans, mid), BF16),
                pltpu.VMEM((layers, 3, 3 * mid, mid), BF16),
                pltpu.VMEM((layers, mid, chans), BF16),
                pltpu.VMEM((layers, 2, mid), F32),
                pltpu.VMEM((layers, 2, mid), F32),
                pltpu.VMEM((layers, chans), F32),
                pltpu.VMEM((layers, chans), F32),
                pltpu.VMEM((size, mid), F32),
                pltpu.VMEM(((rows + 2) * width, 3 * mid), BF16),
                pltpu.VMEM((size, mid), F32),
                pltpu.VMEM((size, mid), BF16),
                pltpu.VMEM((2, 3 * mid, mid), BF16),
                pltpu.VMEM((4, width, mid), F32),
                pltpu.VMEM((layers, 2, width, mid), BF16),
                pltpu.VMEM((layers, 2, width, mid), BF16),
                pltpu.VMEM((2 * layers, 2, mid), F32),
                pltpu.VMEM((2 * layers, n - 1, 2, mid), F32),
                pltpu.VMEM((GROUPS * layers, 2, chans // GROUPS), F32),
                pltpu.VMEM((GROUPS * layers, n - 1, 2, chans // GROUPS), F32),
                dma((rows,)),
                dma((3, layers)),
                dma((4,)),
                dma((layers, 2)),
                dma((layers, 2)),
                dma((2 * layers,)),
                dma((2 * layers,)),
                dma((GROUPS * layers,)),
                dma((GROUPS * layers,)),
            ],
            compiler_params=pltpu.CompilerParams(
                collective_id=0, has_side_effects=True, vmem_limit_bytes=54_400_000
            ),
            name="blocks",
        )(x, w_reduce, taps, w_expand, gain_mid, shift_mid, gain_out, shift_out)
        return pl.pallas_call(
            functools.partial(finish, rows, width),
            out_shape=jax.ShapeDtypeStruct(x.shape, BF16),
            in_specs=[in_vmem] * 3,
            out_specs=anywhere,
            scratch_shapes=[pltpu.VMEM((size, chans // GROUPS), BF16), dma((rows,)), dma((rows,))],
            compiler_params=pltpu.CompilerParams(vmem_limit_bytes=24 * 1024 * 1024),
            name="finish",
        )(ex, last_x, ab)

    placed = (P(("img", "slab"), None, None), P(), P(), P(), P(), P(), P(), P())
    return jax.shard_map(
        local, mesh=mesh, in_specs=placed, out_specs=P(("img", "slab"), None, None), check_vma=False
    )
```

```python
import functools

import jax
import jax.numpy as jnp
from jax import lax
from jax.experimental import pallas as pl
from jax.experimental.pallas import tpu as pltpu
from jax.sharding import PartitionSpec as P

MESH = pl.DeviceIdType.MESH
F32 = jnp.float32
BF16 = jnp.bfloat16
GROUPS = 2


def row_sums(y):
    m, c = y.shape
    y3 = y.reshape(m // 8, 8, c)
    return jnp.sum(y3, axis=0), jnp.sum(y3 * y3, axis=0)


def kernel(
    n, side_y, rows, width, chans, mid, layers,
    x_hbm, wr_hbm, ws_hbm, we_hbm, gm_hbm, sm_hbm, go_hbm, so_hbm,
    ex, x, last_ab,
    wr, ws, we, gm, sm, go, so,
    red, hid, spa, inn, wt, prod,
    halo_out, halo_in, st_out, st_in, se_out, se_in,
    x_sem, w_sem, p_sem, hs_sem, hr_sem, ss_sem, sr_sem, es_sem, er_sem,
):
    me = lax.axis_index("slab")
    count = float(rows * width * n)

    def load(src, dst, sem):
        return pltpu.make_async_copy(src, dst, sem)

    def w_copies(layer):
        return (
            load(wr_hbm.at[layer], wr.at[layer], w_sem.at[0, layer]),
            load(ws_hbm.at[layer], ws.at[layer], w_sem.at[1, layer]),
            load(we_hbm.at[layer], we.at[layer], w_sem.at[2, layer]),
        )

    def x_copy(r):
        return load(x_hbm.at[r], x.at[pl.ds(pl.multiple_of(r * width, width), width)], x_sem.at[r])

    params = ((gm_hbm, gm), (sm_hbm, sm), (go_hbm, go), (so_hbm, so))

    w_copies(0)[0].start()
    early = 4 * rows // 8
    for r in range(early):
        x_copy(r).start()
    for i, (a, b) in enumerate(params):
        load(a, b, p_sem.at[i]).start()
    barrier = pltpu.get_barrier_semaphore()
    for d in range(1, n):
        pl.semaphore_signal(
            barrier, inc=1, device_id={"slab": lax.rem(me + d, n)}, device_id_type=MESH
        )
    pl.delay(400)
    for r in range(early, rows):
        x_copy(r).start()

    def block(r):
        if isinstance(r, int):
            return pl.ds(r * width, width)
        return pl.ds(pl.multiple_of(r * width, width), width)

    def slot_of(side):
        y = lax.rem(me, side_y)
        if side == 0:
            wraps = y == 0
            return jnp.where(wraps, 1 * side_y + 1, 1) - 1
        wraps = y == side_y - 1
        return jnp.where(wraps, n - 1, side_y - 1) - 1

    def distance(d):
        return sum(min(c, side - c) for c, side in ((d // side_y, n // side_y), (d % side_y, side_y)))

    far_first = sorted(range(1, n), key=lambda d: (-distance(d), d))

    def peer(d):
        z, y = me // side_y, me % side_y
        return lax.rem(z + d // side_y, n // side_y) * side_y + lax.rem(y + d % side_y, side_y)

    def send_all(src, dst, slot, send_sem, recv_sem):
        for d in far_first:
            pltpu.make_async_remote_copy(
                src_ref=src.at[slot],
                dst_ref=dst.at[slot, d - 1],
                send_sem=send_sem.at[slot],
                recv_sem=recv_sem.at[slot],
                device_id={"slab": peer(d)},
                device_id_type=MESH,
            ).start()

    def wait_all(dst, slot, sem):
        pltpu.make_async_copy(dst.at[slot], dst.at[slot], sem.at[slot]).wait()

    def pack(s, q):
        return jnp.concatenate(
            [jnp.sum(s, axis=0, keepdims=True), jnp.sum(q, axis=0, keepdims=True)], axis=0
        )

    def coefficients(own, others, gain, shift):
        total = own
        for d in range(n - 1):
            total = total + others[d]
        mean = total[0:1] / count
        var = jnp.maximum(total[1:2] / count - mean * mean, 0.0)
        alpha = lax.rsqrt(var + 1e-05) * gain
        return alpha, shift - mean * alpha

    def reduce_rows(layer, r):
        y = jnp.dot(x[block(r)], wr[layer], preferred_element_type=F32)
        red[block(r)] = y
        return row_sums(y)

    def add2(c, d):
        return c[0] + d[0], c[1] + d[1]

    zero_mid = (jnp.zeros((8, mid), F32), jnp.zeros((8, mid), F32))
    cols = chans // GROUPS
    zero_out = (jnp.zeros((8, cols), F32), jnp.zeros((8, cols), F32))

    def group(g):
        return pl.ds(g * cols, cols)

    w_copies(0)[0].wait()

    carry0 = zero_mid
    for part in (range(early), range(early, rows)):
        for r in part:
            x_copy(r).wait()
        for r in part:
            carry0 = add2(carry0, reduce_rows(0, r))

    for layer in range(layers):
        for j, c in enumerate(w_copies(layer)):
            if (layer, j) != (0, 0):
                c.start()

    pl.semaphore_wait(barrier, n - 1)
    for i, (a, b) in enumerate(params):
        load(a, b, p_sem.at[i]).wait()

    def halo_copy(layer, side):
        peer = me - 1 if side == 0 else me + 1
        return pltpu.make_async_remote_copy(
            src_ref=halo_out.at[layer, side],
            dst_ref=halo_in.at[layer, 1 - side],
            send_sem=hs_sem.at[layer, side],
            recv_sem=hr_sem.at[layer, 1 - side],
            device_id={"slab": peer},
            device_id_type=MESH,
        )

    has_side = (me > 0, me < n - 1)
    for side in range(2):

        @pl.when(jnp.logical_not(has_side[side]))
        def _():
            for layer in range(layers):
                halo_in[layer, side] = jnp.zeros((width, mid), BF16)

    row8 = lax.broadcasted_iota(jnp.int32, (8, mid), 0)

    def put_hidden(slot, h):
        dst = block(slot)
        hid[dst, mid : 2 * mid] = h.astype(BF16)
        before = pltpu.roll(h, 1, 0)
        edge = jnp.where(row8 == 0, 0.0, before[:8])
        hid[dst, 0:mid] = jnp.concatenate([edge, before[8:]], axis=0).astype(BF16)
        after = pltpu.roll(h, width - 1, 0)
        edge = jnp.where(row8 == 7, 0.0, after[-8:])
        hid[dst, 2 * mid : 3 * mid] = jnp.concatenate([after[:-8], edge], axis=0).astype(BF16)

    def layer_body(layer, carry):
        own = pack(*carry)
        k = 2 * layer
        st_out[k] = own
        send_all(st_out, st_in, k, ss_sem, sr_sem)
        local_mean = own[0:1] * (1.0 / (rows * width))
        for side in range(2):
            edge = 0 if side == 0 else rows - 1

            halo_out[layer, side] = (red[block(edge)] - local_mean).astype(BF16)

            @pl.when(has_side[side])
            def _():
                halo_copy(layer, side).start()

        w_copies(layer)[1].wait()

        @pl.loop(0, 3 * mid // 64)
        def _(i):
            at = pl.ds(pl.multiple_of(i * 64, 64), 64)
            outer = ws[layer, 0, at].astype(F32) + ws[layer, 2, at].astype(F32)
            inner = ws[layer, 1, at].astype(F32)
            wt[0, at] = (0.5 * (outer + inner)).astype(BF16)
            wt[1, at] = (0.5 * (outer - inner)).astype(BF16)

        wait_all(st_in, k, sr_sem)
        others = [st_in[k, d] for d in range(n - 1)]
        alpha, beta = coefficients(own, others, gm[layer, 0:1], sm[layer, 0:1])

        def hidden_row(r):
            put_hidden(r + 1, jnp.maximum(red[block(r)] * alpha + beta, 0.0))

        def finish_row(r, carry, lhs, taps, rest):
            y = jnp.dot(lhs, taps, preferred_element_type=F32) + rest
            spa[block(r)] = y
            return add2(carry, row_sums(y))

        hidden_row(0)
        hidden_row(1)
        carry = zero_mid
        for r in range(0, rows, 2):
            a, b = r % 4, r % 4 + 1
            d1, d2 = hid[block(r + 1)], hid[block(r + 2)]
            prod[a] = jnp.dot(d1 + d2, wt[0], preferred_element_type=F32)
            prod[b] = jnp.dot(d2 - d1, wt[1], preferred_element_type=F32)
            if r + 2 < rows:
                hidden_row(r + 2)
                hidden_row(r + 3)
            both = prod[a] + prod[b]
            if r > 0:
                carry = finish_row(r, carry, hid[block(r)] - d2, ws[layer, 0], both)
            else:
                spa[block(r)] = both
            both = prod[a] - prod[b]
            if r + 2 < rows:
                carry = finish_row(r + 1, carry, hid[block(r + 3)] - d1, ws[layer, 2], both)
            else:
                spa[block(r + 1)] = both

        for side in range(2):

            @pl.when(has_side[side])
            def _():
                arrived = halo_in.at[layer, side]
                load(arrived, arrived, hr_sem.at[layer, side]).wait()

        for side in range(2):
            their = st_in[k, slot_of(side)][0:1] * (1.0 / (rows * width))
            y = halo_in[layer, side].astype(F32) + their
            h = jnp.maximum(y * alpha + beta, 0.0)
            put_hidden(0 if side == 0 else rows + 1, jnp.where(has_side[side], h, 0.0))
        lhs = hid[block(0)] - hid[block(2)]
        carry = finish_row(0, carry, lhs, ws[layer, 0], spa[block(0)])
        lhs = hid[block(rows + 1)] - hid[block(rows - 1)]
        carry = finish_row(rows - 1, carry, lhs, ws[layer, 2], spa[block(rows - 1)])

        own = pack(*carry)
        k = 2 * layer + 1
        st_out[k] = own
        send_all(st_out, st_in, k, ss_sem, sr_sem)
        w_copies(layer)[2].wait()

        @pl.loop(0, 13)
        def _(i):
            prod[0] = jnp.dot(hid[block(1)], wt[0], preferred_element_type=F32)

        wait_all(st_in, k, sr_sem)
        others = [st_in[k, d] for d in range(n - 1)]
        alpha, beta = coefficients(own, others, gm[layer, 1:2], sm[layer, 1:2])

        def expand_row(r, g, carry):
            if g == 0:
                inn[block(r)] = jnp.maximum(spa[block(r)] * alpha + beta, 0.0).astype(BF16)
            y = jnp.dot(inn[block(r)], we[layer, :, group(g)], preferred_element_type=F32)
            ex[block(r), group(g)] = y
            return add2(carry, row_sums(y))

        sums = []
        for g in range(GROUPS):
            carry = zero_out
            for r in range(rows):
                carry = expand_row(r, g, carry)
            own = pack(*carry)
            sums.append(own)
            slot = GROUPS * layer + g
            se_out[slot] = own
            send_all(se_out, se_in, slot, es_sem, er_sem)


        @pl.loop(0, 12)
        def _(i):
            prod[0] = jnp.dot(hid[block(1)], wt[0], preferred_element_type=F32)

        carry = zero_mid
        for g in range(GROUPS):
            slot = GROUPS * layer + g
            wait_all(se_in, slot, er_sem)
            others = [se_in[slot, d] for d in range(n - 1)]
            at_layer = pl.ds(layer, 1)
            scale, offset = coefficients(
                sums[g], others, go[at_layer, group(g)], so[at_layer, group(g)]
            )

            def update(r):
                y = (ex[block(r), group(g)] * scale + offset).astype(BF16) + x[block(r), group(g)]
                x[block(r), group(g)] = jnp.maximum(y, jnp.zeros_like(y))

            def middle():
                if g == 0:
                    w_copies(layer + 1)[0].wait()
                carry = zero_mid
                for r in range(rows):
                    update(r)
                    taps = wr[layer + 1, group(g)]
                    y = jnp.dot(x[block(r), group(g)], taps, preferred_element_type=F32)
                    if g > 0:
                        y = y + red[block(r)]
                    red[block(r)] = y
                    if g == GROUPS - 1:
                        carry = add2(carry, row_sums(y))
                return carry

            def last():
                if g < GROUPS - 1:
                    for r in range(rows):
                        update(r)
                else:
                    last_ab[0:1] = scale
                    last_ab[1:2] = offset
                return zero_mid

            carry = lax.cond(layer < layers - 1, middle, last)
        return carry

    lax.fori_loop(0, layers, layer_body, carry0)

    for layer in range(layers):
        for side in range(2):

            @pl.when(has_side[side])
            def _():
                halo_copy(layer, side).wait_send()

        wait_all(st_in, 2 * layer, ss_sem)
        wait_all(st_in, 2 * layer + 1, ss_sem)
        for g in range(GROUPS):
            wait_all(se_in, GROUPS * layer + g, es_sem)


def finish(rows, width, ex, x, ab, out_hbm, out, sem, done_sem):
    alpha, beta = ab[0:1], ab[1:2]
    cols = ab.shape[1]
    done = ex.shape[2] - cols
    ready, left = pl.ds(0, done), pl.ds(done, cols)
    copies = []
    half = rows // 2
    for r in range(0, rows, half):
        at = pl.ds(r, half)
        src = x.at[at, :, ready]
        copies.append(pltpu.make_async_copy(src, out_hbm.at[at, :, ready], done_sem.at[r]))
        copies[-1].start()
    for r in range(rows):
        y = (ex[r, :, left] * alpha + beta).astype(BF16) + x[r, :, left]
        out[r] = jnp.maximum(y, jnp.zeros_like(y))
        copies.append(pltpu.make_async_copy(out.at[r], out_hbm.at[r, :, left], sem.at[r]))
        copies[-1].start()
    for copy in copies:
        copy.wait()


def solution(mesh):
    n = mesh.shape["slab"]
    side_y = 4 if n % 4 == 0 else 1

    def local(x, w_reduce, w_spatial, w_expand, gain_mid, shift_mid, gain_out, shift_out):
        rows, width, chans = x.shape
        layers, _, mid = w_reduce.shape
        taps = w_spatial.reshape(layers, 3, 3 * mid, mid)
        anywhere = pl.BlockSpec(memory_space=pltpu.HBM)
        in_vmem = pl.BlockSpec(memory_space=pltpu.VMEM)
        size = rows * width
        dma = pltpu.SemaphoreType.DMA
        ex, last_x, ab = pl.pallas_call(
            functools.partial(kernel, n, side_y, rows, width, chans, mid, layers),
            out_shape=(
                pltpu.VMEM((size, chans), F32),
                pltpu.VMEM((size, chans), BF16),
                pltpu.VMEM((2, chans // GROUPS), F32),
            ),
            in_specs=[anywhere] * 8,
            out_specs=(in_vmem, in_vmem, in_vmem),
            scratch_shapes=[
                pltpu.VMEM((layers, chans, mid), BF16),
                pltpu.VMEM((layers, 3, 3 * mid, mid), BF16),
                pltpu.VMEM((layers, mid, chans), BF16),
                pltpu.VMEM((layers, 2, mid), F32),
                pltpu.VMEM((layers, 2, mid), F32),
                pltpu.VMEM((layers, chans), F32),
                pltpu.VMEM((layers, chans), F32),
                pltpu.VMEM((size, mid), F32),
                pltpu.VMEM(((rows + 2) * width, 3 * mid), BF16),
                pltpu.VMEM((size, mid), F32),
                pltpu.VMEM((size, mid), BF16),
                pltpu.VMEM((2, 3 * mid, mid), BF16),
                pltpu.VMEM((4, width, mid), F32),
                pltpu.VMEM((layers, 2, width, mid), BF16),
                pltpu.VMEM((layers, 2, width, mid), BF16),
                pltpu.VMEM((2 * layers, 2, mid), F32),
                pltpu.VMEM((2 * layers, n - 1, 2, mid), F32),
                pltpu.VMEM((GROUPS * layers, 2, chans // GROUPS), F32),
                pltpu.VMEM((GROUPS * layers, n - 1, 2, chans // GROUPS), F32),
                dma((rows,)),
                dma((3, layers)),
                dma((4,)),
                dma((layers, 2)),
                dma((layers, 2)),
                dma((2 * layers,)),
                dma((2 * layers,)),
                dma((GROUPS * layers,)),
                dma((GROUPS * layers,)),
            ],
            compiler_params=pltpu.CompilerParams(
                collective_id=0, has_side_effects=True, vmem_limit_bytes=54_400_000
            ),
            name="blocks",
        )(x, w_reduce, taps, w_expand, gain_mid, shift_mid, gain_out, shift_out)
        return pl.pallas_call(
            functools.partial(finish, rows, width),
            out_shape=jax.ShapeDtypeStruct(x.shape, BF16),
            in_specs=[in_vmem] * 3,
            out_specs=anywhere,
            scratch_shapes=[pltpu.VMEM((rows, width, chans // GROUPS), BF16), dma((rows,)), dma((rows,))],
            compiler_params=pltpu.CompilerParams(vmem_limit_bytes=24 * 1024 * 1024),
            name="finish",
        )(ex.reshape(rows, width, chans), last_x.reshape(x.shape), ab)

    placed = (P(("img", "slab"), None, None), P(), P(), P(), P(), P(), P(), P())
    return jax.shard_map(
        local, mesh=mesh, in_specs=placed, out_specs=P(("img", "slab"), None, None), check_vma=False
    )
```
